256 devices in a mesh: tm: 8 (over x_hi, y), space: 32 (over x_lo, z, core).
Axes of the slice: x: 4 (x_hi: 2, x_lo: 2; x = x_hi * 2 + x_lo), y: 4, z: 8, core: 2. Of those that a mesh axis runs over, the one named last changes fastest.
Arguments:
- residual_field: float32 [64, 128, 128, 128], P('tm', 'space'), may hold values from -6 to 6
- eigvec_x: float32 [128, 128], replicated, may hold values from -1 to 1, as said below
- eigvec_y: float32 [128, 128], replicated, may hold values from -1 to 1, as said below
- eigvec_z: float32 [128, 128], replicated, may hold values from -1 to 1, as said below
- eigval_x: float32 [128], replicated, may hold values from 0.0001 to 0.05
- eigval_y: float32 [128], replicated, may hold values from 0.0001 to 0.05
- eigval_z: float32 [128], replicated, may hold values from 0.0001 to 0.05
Outputs:
- update: float32 [64, 128, 128, 128], P('tm', 'space')
The draws below stay inside these ranges and needn't reach their ends.
Inputs may be any that keep to these rules, and one draw needn't show every extreme that they name: `eigvec_x`: an orthogonal matrix. `eigvec_y`: an orthogonal matrix. `eigvec_z`: an orthogonal matrix.
All inputs are finite; a program needn't handle non-finite values.
Results may differ from the reference program's by a relative error of at most 0.00025.
Values sent between devices are 32-bit elements; how exact they have to be, the bound alone decides.
A program may use at most 128 MiB of HBM per device.

```python
import math
import jax
import jax.numpy as jnp
from jax import lax

L = 64
NX = 128
NY = 128
NZ = 128


def orthogonal(key, dimension):

    def reflect(source, matrix):
        vector = jax.random.normal(jax.random.fold_in(key, source), (dimension,), jnp.float32)
        vector = vector / jnp.sqrt(jnp.sum(vector * vector))
        return matrix - 2.0 * jnp.outer(jnp.dot(matrix, vector), vector)
    return lax.fori_loop(0, dimension, reflect, jnp.eye(dimension, dtype=jnp.float32))


def draw_eigvec_x(key, part):
    return orthogonal(jax.random.fold_in(key, 101), NX)


def draw_eigvec_y(key, part):
    return orthogonal(jax.random.fold_in(key, 202), NY)


def draw_eigvec_z(key, part):
    return orthogonal(jax.random.fold_in(key, 303), NZ)


def shard_levels(own_key, dims, cuts, low, top_value):
    gain, own = 1.0, jax.random.fold_in(own_key, 6)
    for position, parts in cuts:
        steps = jnp.exp(jax.random.uniform(jax.random.fold_in(own, position), (parts,), jnp.float32, low / len(cuts), top_value / len(cuts)))
        gain = gain * jnp.repeat(steps, dims[position] // parts).reshape([-1 if axis == position else 1 for axis in range(len(dims))])
    return gain


def gaussian(key, shape, spread, most, pieces=(), held_as=jnp.bfloat16):
    loudness = shard_levels(key, shape, pieces, -0.22, 0.18) if pieces else 1.0
    values = jax.random.normal(key, shape, jnp.float32) * spread * loudness
    return jnp.minimum(jnp.maximum(values, -most), most).astype(held_as)


def setup_inputs(seed: int = 0) -> dict:
    arg_keys = jax.random.split(jax.random.key(seed), 8)
    return {
        "residual_field": gaussian(arg_keys[0], (L, NX, NY, NZ), 1.0, 6.0, ((0, 8), (1, 32)), jnp.float32),
        "eigvec_x": draw_eigvec_x(jax.random.fold_in(arg_keys[7], 71), 0),
        "eigvec_y": draw_eigvec_y(jax.random.fold_in(arg_keys[7], 71), 0),
        "eigvec_z": draw_eigvec_z(jax.random.fold_in(arg_keys[7], 71), 0),
        "eigval_x": jnp.clip(jnp.exp(jax.random.uniform(arg_keys[4], (NX,), jnp.float32, math.log(0.0001), math.log(0.05))), 0.0001, 0.05),
        "eigval_y": jnp.clip(jnp.exp(jax.random.uniform(arg_keys[5], (NY,), jnp.float32, math.log(0.0001), math.log(0.05))), 0.0001, 0.05),
        "eigval_z": jnp.clip(jnp.exp(jax.random.uniform(arg_keys[6], (NZ,), jnp.float32, math.log(0.0001), math.log(0.05))), 0.0001, 0.05),
    }


highest = lax.Precision.HIGHEST
circulant_alpha = 0.01


def spectral_solve(values, shifts, total_steps):
    step_ids = jnp.arange(total_steps, dtype=jnp.int32)
    phases = (step_ids[:, None] * step_ids[None, :]) % total_steps
    angles = (2.0 * math.pi / total_steps) * phases.astype(jnp.float32)
    cosine = jnp.cos(angles)
    sine_table = jnp.sin(angles)
    root_alpha = circulant_alpha ** (1.0 / total_steps)
    powers = root_alpha ** step_ids.astype(jnp.float32)
    flattened = values.reshape(total_steps, -1) * powers[:, None]
    real_part = jnp.dot(cosine, flattened, precision=highest)
    imag_part = -jnp.dot(sine_table, flattened, precision=highest)
    flat_shift = shifts.reshape(1, -1)
    denom_real = 1.0 + flat_shift - root_alpha * cosine[:, 1:2]
    denom_imag = root_alpha * sine_table[:, 1:2]
    modulus = denom_real * denom_real + denom_imag * denom_imag
    quot_real = (real_part * denom_real + imag_part * denom_imag) / modulus
    quot_imag = (imag_part * denom_real - real_part * denom_imag) / modulus
    restored = jnp.dot(cosine, quot_real, precision=highest) - jnp.dot(sine_table, quot_imag, precision=highest)
    restored = restored / (total_steps * powers[:, None])
    return restored.reshape(values.shape)


def reference(residual_field, eigvec_x, eigvec_y, eigvec_z, eigval_x, eigval_y, eigval_z):
    total_steps = residual_field.shape[0]

    def forward_plane(plane):
        plane = jnp.einsum('xyz,zk->xyk', plane, eigvec_z, precision=highest)
        plane = jnp.einsum('xyk,yj->xjk', plane, eigvec_y, precision=highest)
        return jnp.einsum('xjk,xi->ijk', plane, eigvec_x, precision=highest)

    def inverse_plane(plane):
        plane = jnp.einsum('ijk,zk->ijz', plane, eigvec_z, precision=highest)
        plane = jnp.einsum('ijz,yj->iyz', plane, eigvec_y, precision=highest)
        return jnp.einsum('iyz,xi->xyz', plane, eigvec_x, precision=highest)

    coeffs = lax.map(forward_plane, residual_field)
    shift_yz = eigval_y[:, None] + eigval_z[None, :]

    def solve_slab(source):
        slab = lax.dynamic_index_in_dim(coeffs, source, 1, keepdims=False)
        shift_x = lax.dynamic_index_in_dim(eigval_x, source, 0, keepdims=False)
        return spectral_solve(slab, shift_x + shift_yz, total_steps)

    solved = lax.map(solve_slab, jnp.arange(eigval_x.shape[0], dtype=jnp.int32))
    solved = jnp.moveaxis(solved, 0, 1)
    return lax.map(inverse_plane, solved)
```

```python
import functools

import jax
import jax.numpy as jnp
from jax import lax
from jax.experimental import pallas as pl
from jax.experimental.pallas import tpu as pltpu
from jax.sharding import PartitionSpec as P

ALPHA = 0.01
CHUNKS = 4
F32 = jnp.float32
BF16 = jnp.bfloat16
MESH = pl.DeviceIdType.MESH


def halves(v):
    high = v.astype(BF16)
    return high, (v - high.astype(F32)).astype(BF16)


def left_weight(w):
    high, low = halves(w)
    return jnp.concatenate(
        [jnp.concatenate([high, high], 1), jnp.concatenate([low, low], 1)], 0
    )


def right_weight(w):
    half = jnp.concatenate(list(halves(w)), 1)
    return jnp.concatenate([half, half], 0)


def left_dot(weight, v):
    rows = v.shape[0]
    out = jnp.dot(weight, jnp.concatenate(list(halves(v)), 0), preferred_element_type=F32)
    return out[:rows] + out[rows:]


def right_dot(v, weight):
    columns = v.shape[1]
    out = jnp.dot(jnp.concatenate(list(halves(v)), 1), weight, preferred_element_type=F32)
    return out[:, :columns] + out[:, columns:]


def exchange_kernel(
    field, vec_x, vec_y, vec_z, val_x, val_y, val_z,
    returned, inv_y, inv_z,
    sent, landed, states, carries, solved, fwd_x, bwd_x, fwd_y, fwd_z, decay,
    s_send, s_recv, c_send, c_recv, b_send, b_recv,
):
    steps, rows, size, lanes = field.shape
    tm_count, space_count = lax.axis_size("tm"), lax.axis_size("space")
    me_t, me = lax.axis_index("tm"), lax.axis_index("space")
    place_x, place_z, core = me // 16, (me // 2) % 8, me % 2
    block = size // CHUNKS

    def partner(n):
        level = n // 4
        away = ((level + 1) // 2) * (2 * (level % 2) - 1)
        to_x = (place_x + (n // 2) % 2) % 2
        to_z = (place_z + away + 8) % 8
        return to_x * 16 + to_z * 2 + (core + n % 2) % 2

    barrier = pltpu.get_barrier_semaphore()

    @pl.loop(1, space_count)
    def _(n):
        pl.semaphore_signal(barrier, 1, device_id={"space": partner(n)}, device_id_type=MESH)

    @pl.loop(1, tm_count)
    def _(m):
        to = (me_t + m) % tm_count
        pl.semaphore_signal(barrier, 1, device_id={"tm": to}, device_id_type=MESH)

    fwd_z[...] = right_weight(vec_z[...])
    fwd_y[...] = left_weight(vec_y[...].T)

    sent_rows = sent.reshape(rows * size * steps, lanes)
    landed_rows = landed.reshape(CHUNKS * size * steps, lanes)
    solved_rows = solved.reshape(CHUNKS * size * steps, lanes)

    @pl.loop(0, rows)
    def _(x):
        for pair in range(steps // 2):
            plane = field[2 * pair : 2 * pair + 2, x].reshape(2 * size, lanes)
            plane = right_dot(plane, fwd_z[...])
            plane = jnp.concatenate([plane[:size], plane[size:]], 1)
            plane = left_dot(fwd_y[...], plane)
            for k in range(2):
                at = pl.ds(x * size * steps + 2 * pair + k, size, stride=steps)
                sent_rows[at, :] = plane[:, k * lanes : (k + 1) * lanes]

    pl.semaphore_wait(barrier, space_count + tm_count - 2)

    @pl.loop(0, CHUNKS)
    def _(c):
        @pl.loop(1, space_count)
        def _(n):
            to = partner(n)
            pltpu.make_async_remote_copy(
                sent.at[:, c * block + to],
                landed.at[c, pl.ds(rows * me, rows)],
                s_send.at[c],
                s_recv.at[c],
                device_id={"space": to},
                device_id_type=MESH,
            ).start()

    fwd_x[...] = left_weight(vec_x[...].T)
    bwd_x[...] = left_weight(vec_x[...])
    inv_y[...] = left_weight(vec_y[...])
    inv_z[...] = right_weight(vec_z[...].T)
    column_x = jnp.broadcast_to(val_x[...], (size, lanes)).T

    def whole(c):
        return landed.at[c, pl.ds(0, size - rows)]

    def whole_back(c):
        return returned.at[:, pl.ds(c * block, block - 1)]

    @pl.loop(0, CHUNKS)
    def _(c):
        landed[c, pl.ds(rows * me, rows)] = sent[:, c * block + me]
        shift = column_x + (val_y[c * block + me] + val_z[...])
        decay[...] = 1.0 / (1.0 + shift)
        pltpu.make_async_copy(whole(c), whole(c), s_recv.at[c]).wait()
        state = jnp.zeros((size, lanes), F32)
        for pair in range(steps // 2):
            first = c * size * steps + 2 * pair
            plane = jnp.concatenate(
                [landed_rows[pl.ds(first + k, size, stride=steps), :] for k in range(2)], 1
            )
            plane = left_dot(fwd_x[...], plane)
            for k in range(2):
                state = decay[...] * (plane[:, k * lanes : (k + 1) * lanes] + state)
                states[c, 2 * pair + k] = state

        @pl.loop(1, tm_count)
        def _(m):
            pltpu.make_async_remote_copy(
                states.at[c, steps - 1],
                carries.at[c, m - 1],
                c_send.at[c],
                c_recv.at[c],
                device_id={"tm": (me_t + m) % tm_count},
                device_id_type=MESH,
            ).start()

        pltpu.make_async_copy(carries.at[c], carries.at[c], c_recv.at[c]).wait()
        a = decay[...]
        a8 = a
        for _ in range(3):
            a8 = a8 * a8
        whole_decay = a8
        for _ in range(3):
            whole_decay = whole_decay * whole_decay
        total = ALPHA * states[c, steps - 1]
        for m in range(tm_count - 1, 0, -1):
            weight = jnp.where(me_t < m, ALPHA, 1.0).astype(F32)
            total = total * a8 + weight * carries[c, m - 1]
        past = a * (total / (1.0 - ALPHA * whole_decay))
        for pair in range(steps // 2):
            planes = []
            for k in range(2):
                planes.append(states[c, 2 * pair + k] + past)
                past = past * a
            plane = left_dot(bwd_x[...], jnp.concatenate(planes, 1))
            for k in range(2):
                at = pl.ds(c * size * steps + 2 * pair + k, size, stride=steps)
                solved_rows[at, :] = plane[:, k * lanes : (k + 1) * lanes]

        @pl.loop(1, space_count)
        def _(n):
            to = partner(n)
            pltpu.make_async_remote_copy(
                solved.at[c, pl.ds(rows * to, rows)],
                returned.at[:, c * block + me],
                b_send.at[c],
                b_recv.at[c],
                device_id={"space": to},
                device_id_type=MESH,
            ).start()

        returned[:, c * block + me] = solved[c, pl.ds(rows * me, rows)]

    @pl.loop(0, CHUNKS)
    def _(c):
        pltpu.make_async_copy(whole(c), whole(c), s_send.at[c]).wait()
        pltpu.make_async_copy(carries.at[c], carries.at[c], c_send.at[c]).wait()
        pltpu.make_async_copy(whole_back(c), whole_back(c), b_recv.at[c]).wait()
        pltpu.make_async_copy(whole_back(c), whole_back(c), b_send.at[c]).wait()


def inverse_kernel(returned, inv_y, inv_z, update):
    _, size, steps, lanes = returned.shape
    rows = returned.reshape(size * steps, lanes)
    for pair in range(steps // 2):
        plane = jnp.concatenate(
            [rows[pl.ds(2 * pair + k, size, stride=steps), :] for k in range(2)], 1
        )
        plane = left_dot(inv_y[...], plane)
        plane = jnp.concatenate([plane[:, :lanes], plane[:, lanes:]], 0)
        plane = right_dot(plane, inv_z[...])
        update[2 * pair : 2 * pair + 2, 0] = plane.reshape(2, size, lanes)


def shards(residual_field, eigvec_x, eigvec_y, eigvec_z, eigval_x, eigval_y, eigval_z):
    steps, rows, size, lanes = residual_field.shape
    tm_count = lax.axis_size("tm")
    vmem = pl.BlockSpec(memory_space=pltpu.VMEM)
    weight = jax.ShapeDtypeStruct((2 * size, 2 * size), BF16)
    dma = pltpu.SemaphoreType.DMA((CHUNKS,))
    returned, inv_y, inv_z = pl.pallas_call(
        exchange_kernel,
        out_shape=(jax.ShapeDtypeStruct((rows, size, steps, lanes), F32), weight, weight),
        in_specs=[vmem] * 5 + [pl.BlockSpec(memory_space=pltpu.SMEM), vmem],
        out_specs=(vmem, vmem, vmem),
        scratch_shapes=[
            pltpu.VMEM((rows, size, steps, lanes), F32),
            pltpu.VMEM((CHUNKS, size, steps, lanes), F32),
            pltpu.VMEM((CHUNKS, steps, size, lanes), F32),
            pltpu.VMEM((CHUNKS, tm_count - 1, size, lanes), F32),
            pltpu.VMEM((CHUNKS, size, steps, lanes), F32),
        ]
        + [pltpu.VMEM((2 * size, 2 * size), BF16)] * 4
        + [pltpu.VMEM((size, lanes), F32)]
        + [dma] * 6,
        compiler_params=pltpu.CompilerParams(
            collective_id=0, has_side_effects=True, vmem_limit_bytes=48 * 1024 * 1024
        ),
        name="exchange",
    )(
        residual_field,
        eigvec_x,
        eigvec_y,
        eigvec_z,
        eigval_x.reshape(1, -1),
        eigval_y,
        eigval_z.reshape(1, -1),
    )
    fixed = pl.BlockSpec((2 * size, 2 * size), lambda x: (0, 0))
    return pl.pallas_call(
        inverse_kernel,
        grid=(rows,),
        out_shape=jax.ShapeDtypeStruct((steps, rows, size, lanes), F32),
        in_specs=[pl.BlockSpec((1, size, steps, lanes), lambda x: (x, 0, 0, 0)), fixed, fixed],
        out_specs=pl.BlockSpec((steps, 1, size, lanes), lambda x: (0, x, 0, 0)),
        compiler_params=pltpu.CompilerParams(vmem_limit_bytes=16 * 1024 * 1024),
        name="inverse",
    )(returned, inv_y, inv_z)


def solution(mesh):
    placed = (P("tm", "space", None, None), P(), P(), P(), P(), P(), P())
    return jax.shard_map(
        shards, mesh=mesh, in_specs=placed, out_specs=P("tm", "space", None, None), check_vma=False
    )
```

```python
import functools

import jax
import jax.numpy as jnp
from jax import lax
from jax.experimental import pallas as pl
from jax.experimental.pallas import tpu as pltpu
from jax.sharding import PartitionSpec as P

ALPHA = 0.01
CHUNKS = 4
F32 = jnp.float32
BF16 = jnp.bfloat16
MESH = pl.DeviceIdType.MESH


def halves(v):
    high = v.astype(BF16)
    return high, (v - high.astype(F32)).astype(BF16)


def left_weight(w):
    high, low = halves(w)
    return jnp.concatenate(
        [jnp.concatenate([high, high], 1), jnp.concatenate([low, low], 1)], 0
    )


def right_weight(w):
    half = jnp.concatenate(list(halves(w)), 1)
    return jnp.concatenate([half, half], 0)


def left_dot(weight, v):
    rows = v.shape[0]
    out = jnp.dot(weight, jnp.concatenate(list(halves(v)), 0), preferred_element_type=F32)
    return out[:rows] + out[rows:]


def right_dot(v, weight):
    columns = v.shape[1]
    out = jnp.dot(jnp.concatenate(list(halves(v)), 1), weight, preferred_element_type=F32)
    return out[:, :columns] + out[:, columns:]


def exchange_kernel(
    field_hbm, vec_x_hbm, vec_y_hbm, vec_z_hbm, val_x_hbm, val_y_hbm, val_z_hbm,
    turned_hbm,
    field, vec_x, vec_y, vec_z, val_x, val_y, val_z,
    sent, landed, states, carries, solved, returned, turned, fwd_x, bwd_x, fwd_y, fwd_z, inv_z, decay,
    load, s_send, s_recv, c_send, c_recv, b_send, b_recv, store,
):
    steps, rows, size, lanes = field.shape
    tm_count, space_count = lax.axis_size("tm"), lax.axis_size("space")
    me_t, me = lax.axis_index("tm"), lax.axis_index("space")
    block = size // CHUNKS

    place_x, place_z, core = lax.div(me, 16), lax.rem(lax.div(me, 2), 8), lax.rem(me, 2)
    along_x = [place_x * 16, 16 - place_x * 16]
    along_core = [core, 1 - core]
    partners = []
    for away in (0, 1, -1, 2, -2, 3, -3, 4):
        at_z = lax.rem(place_z + (away + 8), 8) * 2
        for at_x in along_x:
            partners += [at_x + at_z + at_core for at_core in along_core]
    partners = partners[1:]
    followers = [lax.rem(me_t + m, tm_count) for m in range(1, tm_count)]

    loads = [
        pltpu.make_async_copy(source, target, load.at[k])
        for k, (source, target) in enumerate(
            [(vec_y_hbm, vec_y)]
            + [(field_hbm.at[:, x], field.at[:, x]) for x in range(rows)]
            + [
                (vec_z_hbm, vec_z),
                (vec_x_hbm, vec_x),
                (val_x_hbm, val_x),
                (val_y_hbm, val_y),
                (val_z_hbm, val_z),
            ]
        )
    ]
    for copy in loads:
        copy.start()

    barrier = pltpu.get_barrier_semaphore()
    for to in partners:
        pl.semaphore_signal(barrier, 1, device_id={"space": to}, device_id_type=MESH)
    for to in followers:
        pl.semaphore_signal(barrier, 1, device_id={"tm": to}, device_id_type=MESH)

    sent_rows = sent.reshape(rows * size * steps, lanes)
    landed_rows = landed.reshape(CHUNKS * size * steps, lanes)
    solved_rows = solved.reshape(CHUNKS * size * steps, lanes)

    loads[0].wait()
    fwd_y[...] = left_weight(vec_y[...].T)
    for x in range(rows):
        loads[1 + x].wait()
        for pair in range(steps // 2):
            plane = jnp.concatenate([field[2 * pair + k, x] for k in range(2)], 1)
            plane = left_dot(fwd_y[...], plane)
            for k in range(2):
                at = pl.ds(x * size * steps + 2 * pair + k, size, stride=steps)
                sent_rows[at, :] = plane[:, k * lanes : (k + 1) * lanes]
    loads[1 + rows].wait()
    fwd_z[...] = right_weight(vec_z[...])

    def forward_z(c):
        for x in range(rows):
            part = sent[x, pl.ds(c * block, block)].reshape(block * steps, lanes)
            part = right_dot(part, fwd_z[...])
            sent[x, pl.ds(c * block, block)] = part.reshape(block, steps, lanes)

    forward_z(0)
    pl.semaphore_wait(barrier, space_count + tm_count - 2)

    @pl.loop(0, CHUNKS)
    def _(c):
        for to in partners:
            pltpu.make_async_remote_copy(
                sent.at[:, c * block + to],
                landed.at[c, pl.ds(rows * me, rows)],
                s_send.at[c],
                s_recv.at[c],
                device_id={"space": to},
                device_id_type=MESH,
            ).start()

        @pl.when(c < CHUNKS - 1)
        def _():
            forward_z(c + 1)

    for copy in loads[2 + rows :]:
        copy.wait()
    fwd_x[...] = left_weight(vec_x[...].T)
    bwd_x[...] = left_weight(vec_x[...])
    inv_z[...] = right_weight(vec_z[...].T)
    column_x = jnp.broadcast_to(val_x[...], (size, lanes)).T

    def whole(c):
        return landed.at[c, pl.ds(0, size - rows)]

    def stored(c):
        part = pl.ds(c * block, block)
        return pltpu.make_async_copy(turned.at[:, part], turned_hbm.at[:, part], store.at[c])

    def whole_back(c):
        return returned.at[:, pl.ds(c * block, block - 1)]

    @pl.loop(0, CHUNKS)
    def _(c):
        landed[c, pl.ds(rows * me, rows)] = sent[:, c * block + me]
        shift = column_x + (val_y[c * block + me] + val_z[...])
        decay[...] = 1.0 / (1.0 + shift)
        pltpu.make_async_copy(whole(c), whole(c), s_recv.at[c]).wait()
        state = jnp.zeros((size, lanes), F32)
        for pair in range(steps // 2):
            first = c * size * steps + 2 * pair
            plane = jnp.concatenate(
                [landed_rows[pl.ds(first + k, size, stride=steps), :] for k in range(2)], 1
            )
            plane = left_dot(fwd_x[...], plane)
            for k in range(2):
                state = decay[...] * (plane[:, k * lanes : (k + 1) * lanes] + state)
                states[c, 2 * pair + k] = state

        for m, to in enumerate(followers):
            pltpu.make_async_remote_copy(
                states.at[c, steps - 1],
                carries.at[c, m],
                c_send.at[c],
                c_recv.at[c],
                device_id={"tm": to},
                device_id_type=MESH,
            ).start()

        pltpu.make_async_copy(carries.at[c], carries.at[c], c_recv.at[c]).wait()
        a = decay[...]
        a8 = a
        for _ in range(3):
            a8 = a8 * a8
        whole_decay = a8
        for _ in range(3):
            whole_decay = whole_decay * whole_decay
        total = ALPHA * states[c, steps - 1]
        for m in range(tm_count - 1, 0, -1):
            weight = jnp.where(me_t < m, ALPHA, 1.0).astype(F32)
            total = total * a8 + weight * carries[c, m - 1]
        past = a * (total / (1.0 - ALPHA * whole_decay))
        for pair in range(steps // 2):
            planes = []
            for k in range(2):
                planes.append(states[c, 2 * pair + k] + past)
                past = past * a
            plane = left_dot(bwd_x[...], jnp.concatenate(planes, 1))
            for k in range(2):
                at = pl.ds(c * size * steps + 2 * pair + k, size, stride=steps)
                solved_rows[at, :] = plane[:, k * lanes : (k + 1) * lanes]

        for to in partners:
            pltpu.make_async_remote_copy(
                solved.at[c, pl.ds(rows * to, rows)],
                returned.at[:, c * block + me],
                b_send.at[c],
                b_recv.at[c],
                device_id={"space": to},
                device_id_type=MESH,
            ).start()

        returned[:, c * block + me] = solved[c, pl.ds(rows * me, rows)]

    @pl.loop(0, CHUNKS)
    def _(c):
        pltpu.make_async_copy(whole(c), whole(c), s_send.at[c]).wait()
        pltpu.make_async_copy(carries.at[c], carries.at[c], c_send.at[c]).wait()
        pltpu.make_async_copy(whole_back(c), whole_back(c), b_recv.at[c]).wait()
        for x in range(rows):
            part = returned[x, pl.ds(c * block, block)].reshape(block * steps, lanes)
            part = right_dot(part, inv_z[...])
            turned[x, pl.ds(c * block, block)] = part.reshape(block, steps, lanes)
        stored(c).start()
        pltpu.make_async_copy(whole_back(c), whole_back(c), b_send.at[c]).wait()

    @pl.loop(0, CHUNKS)
    def _(c):
        stored(c).wait()


def inverse_kernel(turned_hbm, vec_y_hbm, update_hbm, turned, vec_y, update, inv_y, load, store):
    count, size, steps, lanes = turned.shape
    loads = [pltpu.make_async_copy(vec_y_hbm, vec_y, load.at[count])] + [
        pltpu.make_async_copy(turned_hbm.at[x], turned.at[x], load.at[x]) for x in range(count)
    ]
    for copy in loads:
        copy.start()
    loads[0].wait()
    inv_y[...] = left_weight(vec_y[...])
    rows = turned.reshape(count * size * steps, lanes)
    stores = []
    for x in range(count):
        loads[1 + x].wait()
        for pair in range(steps // 2):
            first = x * size * steps + 2 * pair
            plane = jnp.concatenate(
                [rows[pl.ds(first + k, size, stride=steps), :] for k in range(2)], 1
            )
            plane = left_dot(inv_y[...], plane)
            for k in range(2):
                update[2 * pair + k, x] = plane[:, k * lanes : (k + 1) * lanes]
            part = pl.ds(2 * pair, 2)
            stores.append(
                pltpu.make_async_copy(
                    update.at[part, x], update_hbm.at[part, x], store.at[len(stores)]
                )
            )
            stores[-1].start()
    for copy in stores:
        copy.wait()


def shards(residual_field, eigvec_x, eigvec_y, eigvec_z, eigval_x, eigval_y, eigval_z):
    steps, rows, size, lanes = residual_field.shape
    tm_count = lax.axis_size("tm")
    hbm = pl.BlockSpec(memory_space=pltpu.HBM)
    square = pltpu.VMEM((size, size), F32)
    spread = pltpu.VMEM((rows, size, steps, lanes), F32)
    slots = pltpu.VMEM((CHUNKS, size, steps, lanes), F32)
    dma = pltpu.SemaphoreType.DMA((CHUNKS,))
    turned = pl.pallas_call(
        exchange_kernel,
        out_shape=jax.ShapeDtypeStruct((rows, size, steps, lanes), F32),
        in_specs=[hbm] * 7,
        out_specs=hbm,
        scratch_shapes=[
            pltpu.VMEM((steps, rows, size, lanes), F32),
            square,
            square,
            square,
            pltpu.VMEM((1, lanes), F32),
            pltpu.SMEM((size,), F32),
            pltpu.VMEM((1, lanes), F32),
            spread,
            slots,
            pltpu.VMEM((CHUNKS, steps, size, lanes), F32),
            pltpu.VMEM((CHUNKS, tm_count - 1, size, lanes), F32),
            slots,
            spread,
            spread,
        ]
        + [pltpu.VMEM((2 * size, 2 * size), BF16)] * 5
        + [square]
        + [pltpu.SemaphoreType.DMA((6 + rows,))]
        + [dma] * 7,
        compiler_params=pltpu.CompilerParams(
            collective_id=0, has_side_effects=True, vmem_limit_bytes=58000 * 1024
        ),
        name="exchange",
    )(
        residual_field,
        eigvec_x,
        eigvec_y,
        eigvec_z,
        eigval_x.reshape(1, -1),
        eigval_y,
        eigval_z.reshape(1, -1),
    )
    return pl.pallas_call(
        inverse_kernel,
        out_shape=jax.ShapeDtypeStruct((steps, rows, size, lanes), F32),
        in_specs=[hbm, hbm],
        out_specs=hbm,
        scratch_shapes=[
            spread,
            square,
            pltpu.VMEM((steps, rows, size, lanes), F32),
            pltpu.VMEM((2 * size, 2 * size), BF16),
            pltpu.SemaphoreType.DMA((rows + 1,)),
            pltpu.SemaphoreType.DMA((rows * steps // 2,)),
        ],
        compiler_params=pltpu.CompilerParams(vmem_limit_bytes=60000 * 1024),
        name="inverse",
    )(turned, eigvec_y)


def solution(mesh):
    placed = (P("tm", "space", None, None), P(), P(), P(), P(), P(), P())
    return jax.shard_map(
        shards, mesh=mesh, in_specs=placed, out_specs=P("tm", "space", None, None), check_vma=False
    )
```

```python
import functools

import jax
import jax.numpy as jnp
from jax import lax
from jax.experimental import pallas as pl
from jax.experimental.pallas import tpu as pltpu
from jax.sharding import PartitionSpec as P

ALPHA = 0.01
CHUNKS = 4
GROUP = 2
LAST_ORDER = (0, 1, 2, 3, 4, 7, 5, 6)
F32 = jnp.float32
BF16 = jnp.bfloat16
MESH = pl.DeviceIdType.MESH


def halves(v):
    high = v.astype(BF16)
    return high, (v - high.astype(F32)).astype(BF16)


def left_weight(w):
    high, low = halves(w)
    return jnp.concatenate(
        [jnp.concatenate([high, high], 1), jnp.concatenate([low, low], 1)], 0
    )


def right_weight(w):
    half = jnp.concatenate(list(halves(w)), 1)
    return jnp.concatenate([half, half], 0)


def left_dot(weight, v):
    rows = v.shape[0]
    out = jnp.dot(weight, jnp.concatenate(list(halves(v)), 0), preferred_element_type=F32)
    return out[:rows] + out[rows:]


def right_dot(v, weight):
    columns = v.shape[1]
    out = jnp.dot(jnp.concatenate(list(halves(v)), 1), weight, preferred_element_type=F32)
    return out[:, :columns] + out[:, columns:]


def stacked(pair):
    columns = pair.shape[1] // 2
    return jnp.concatenate([pair[:, :columns], pair[:, columns:]], 0)


def exchange_kernel(
    field_hbm, vec_x_hbm, vec_y_hbm, vec_z_hbm, val_x_hbm, val_y_hbm, val_z_hbm,
    turned,
    field, vec_x, vec_y, vec_z, val_x, val_y, val_z,
    sent, landed, states, carries, solved, fwd_x, bwd_x, fwd_y, fwd_z, inv_z, decay,
    load, s_send, s_recv, c_send, c_recv, b_send, b_recv, store,
):
    steps, rows, size, lanes = field.shape
    tm_count, space_count = lax.axis_size("tm"), lax.axis_size("space")
    me_t, me = lax.axis_index("tm"), lax.axis_index("space")
    block = size // CHUNKS

    place_x, place_z, core = lax.div(me, 16), lax.rem(lax.div(me, 2), 8), lax.rem(me, 2)
    along_x = [place_x * 16, 16 - place_x * 16]
    along_core = [core, 1 - core]
    partners = []
    for away in (0, 1, -1, 2, -2, 3, -3, 4):
        at_z = lax.rem(place_z + (away + 8), 8) * 2
        for at_x in along_x:
            partners += [at_x + at_z + at_core for at_core in along_core]
    partners = partners[1:]
    followers = [lax.rem(me_t + m, tm_count) for m in range(1, tm_count)]

    loads = [
        pltpu.make_async_copy(source, target, load.at[k])
        for k, (source, target) in enumerate(
            [(vec_y_hbm, vec_y)]
            + [(field_hbm.at[:, x], field.at[:, x]) for x in range(rows)]
            + [
                (vec_z_hbm, vec_z),
                (vec_x_hbm, vec_x),
                (val_x_hbm, val_x),
                (val_y_hbm, val_y),
                (val_z_hbm, val_z),
            ]
        )
    ]
    for copy in loads:
        copy.start()

    barrier = pltpu.get_barrier_semaphore()
    for to in partners:
        pl.semaphore_signal(barrier, 1, device_id={"space": to}, device_id_type=MESH)
    for to in followers:
        pl.semaphore_signal(barrier, 1, device_id={"tm": to}, device_id_type=MESH)

    sent_rows = sent.reshape(rows * size * steps, lanes)
    landed_rows = landed.reshape(CHUNKS * size * steps, lanes)
    solved_rows = solved.reshape(CHUNKS * size * steps, lanes)

    loads[0].wait()
    fwd_y[...] = left_weight(vec_y[...].T)
    for x in range(rows):
        loads[1 + x].wait()
        for pair in range(steps // 2):
            plane = jnp.concatenate([field[2 * pair + k, x] for k in range(2)], 1)
            plane = left_dot(fwd_y[...], plane)
            for k in range(2):
                at = pl.ds(x * size * steps + 2 * pair + k, size, stride=steps)
                sent_rows[at, :] = plane[:, k * lanes : (k + 1) * lanes]
    pl.semaphore_wait(barrier, space_count + tm_count - 2)

    @pl.loop(0, CHUNKS)
    def _(c):
        for to in partners:
            pltpu.make_async_remote_copy(
                sent.at[:, c * block + to],
                landed.at[c, pl.ds(rows * me, rows)],
                s_send.at[c],
                s_recv.at[c],
                device_id={"space": to},
                device_id_type=MESH,
            ).start()

    for copy in loads[1 + rows :]:
        copy.wait()
    fwd_z[...] = right_weight(vec_z[...])
    fwd_x[...] = left_weight(vec_x[...].T)
    bwd_x[...] = left_weight(vec_x[...])
    inv_z[...] = right_weight(vec_z[...].T)
    column_x = jnp.broadcast_to(val_x[...], (size, lanes)).T

    def whole(c):
        return landed.at[c, pl.ds(0, size - rows)]

    def own_block(c):
        return pltpu.make_async_copy(
            solved.at[c, pl.ds(rows * me, rows)], turned.at[:, c * block + me], store.at[c]
        )

    def whole_back(c):
        return turned.at[:, pl.ds(c * block, block - 1)]

    @pl.loop(0, CHUNKS)
    def _(c):
        landed[c, pl.ds(rows * me, rows)] = sent[:, c * block + me]
        shift = column_x + (val_y[c * block + me] + val_z[...])
        decay[...] = 1.0 / (1.0 + shift)
        pltpu.make_async_copy(whole(c), whole(c), s_recv.at[c]).wait()
        state = jnp.zeros((size, lanes), F32)
        for pair in range(steps // 2):
            first = c * size * steps + 2 * pair
            plane = jnp.concatenate(
                [landed_rows[pl.ds(first + k, size, stride=steps), :] for k in range(2)], 1
            )
            plane = stacked(left_dot(fwd_x[...], plane))
            plane = right_dot(plane, fwd_z[...])
            for k in range(2):
                state = decay[...] * (plane[k * size : (k + 1) * size] + state)
                states[c, 2 * pair + k] = state

        for m, to in enumerate(followers):
            pltpu.make_async_remote_copy(
                states.at[c, steps - 1],
                carries.at[c, m],
                c_send.at[c],
                c_recv.at[c],
                device_id={"tm": to},
                device_id_type=MESH,
            ).start()

        pltpu.make_async_copy(carries.at[c], carries.at[c], c_recv.at[c]).wait()
        a = decay[...]
        a8 = a
        for _ in range(3):
            a8 = a8 * a8
        whole_decay = a8
        for _ in range(3):
            whole_decay = whole_decay * whole_decay
        total = ALPHA * states[c, steps - 1]
        for m in range(tm_count - 1, 0, -1):
            weight = jnp.where(me_t < m, ALPHA, 1.0).astype(F32)
            total = total * a8 + weight * carries[c, m - 1]
        past = a * (total / (1.0 - ALPHA * whole_decay))
        for pair in range(steps // 2):
            planes = []
            for k in range(2):
                planes.append(states[c, 2 * pair + k] + past)
                past = past * a
            plane = stacked(left_dot(bwd_x[...], jnp.concatenate(planes, 1)))
            plane = right_dot(plane, inv_z[...])
            for k in range(2):
                at = pl.ds(c * size * steps + 2 * pair + k, size, stride=steps)
                solved_rows[at, :] = plane[k * size : (k + 1) * size]

        def send_back(to):
            pltpu.make_async_remote_copy(
                solved.at[c, pl.ds(rows * to, rows)],
                turned.at[:, c * block + me],
                b_send.at[c],
                b_recv.at[c],
                device_id={"space": to},
                device_id_type=MESH,
            ).start()

        @pl.when(c < CHUNKS - 1)
        def _():
            for to in partners:
                send_back(to)

        @pl.when(c == CHUNKS - 1)
        def _():
            for at_z in LAST_ORDER:
                for at_x in along_x:
                    for at_core in along_core:
                        to = at_x + 2 * at_z + at_core
                        if at_x is along_x[0] and at_core is along_core[0]:
                            pl.when(place_z != at_z)(functools.partial(send_back, to))
                        else:
                            send_back(to)

        own_block(c).start()

    @pl.loop(0, CHUNKS)
    def _(c):
        own_block(c).wait()
        pltpu.make_async_copy(whole(c), whole(c), s_send.at[c]).wait()
        pltpu.make_async_copy(carries.at[c], carries.at[c], c_send.at[c]).wait()
        pltpu.make_async_copy(whole_back(c), whole_back(c), b_recv.at[c]).wait()
        pltpu.make_async_copy(whole(c), whole(c), b_send.at[c]).wait()


def inverse_kernel(turned_hbm, vec_y_hbm, update_hbm, turned, vec_y, update, inv_y, load, store):
    count, size, steps, lanes = turned.shape
    loads = [pltpu.make_async_copy(vec_y_hbm, vec_y, load.at[count])] + [
        pltpu.make_async_copy(turned_hbm.at[x], turned.at[x], load.at[x]) for x in range(count)
    ]
    for copy in loads:
        copy.start()
    loads[0].wait()
    inv_y[...] = left_weight(vec_y[...])
    rows = turned.reshape(count * size * steps, lanes)
    stores = []
    for group in range(0, count, GROUP):
        for copy in loads[1 + group : 1 + group + GROUP]:
            copy.wait()
        for x in range(group, group + GROUP):
            for pair in range(steps // 2):
                first = x * size * steps + 2 * pair
                plane = jnp.concatenate(
                    [rows[pl.ds(first + k, size, stride=steps), :] for k in range(2)], 1
                )
                plane = left_dot(inv_y[...], plane)
                for k in range(2):
                    update[2 * pair + k, x] = plane[:, k * lanes : (k + 1) * lanes]
        for x in range(group, group + GROUP):
            part = update_hbm.at[:, x]
            stores.append(pltpu.make_async_copy(update.at[:, x], part, store.at[x]))
            stores[-1].start()
    for copy in stores:
        copy.wait()


def shards(residual_field, eigvec_x, eigvec_y, eigvec_z, eigval_x, eigval_y, eigval_z):
    steps, rows, size, lanes = residual_field.shape
    tm_count = lax.axis_size("tm")
    hbm = pl.BlockSpec(memory_space=pltpu.HBM)
    square = pltpu.VMEM((size, size), F32)
    spread = pltpu.VMEM((rows, size, steps, lanes), F32)
    slots = pltpu.VMEM((CHUNKS, size, steps, lanes), F32)
    dma = pltpu.SemaphoreType.DMA((CHUNKS,))
    turned = pl.pallas_call(
        exchange_kernel,
        out_shape=jax.ShapeDtypeStruct((rows, size, steps, lanes), F32),
        in_specs=[hbm] * 7,
        out_specs=hbm,
        scratch_shapes=[
            pltpu.VMEM((steps, rows, size, lanes), F32),
            square,
            square,
            square,
            pltpu.VMEM((1, lanes), F32),
            pltpu.SMEM((size,), F32),
            pltpu.VMEM((1, lanes), F32),
            spread,
            slots,
            pltpu.VMEM((CHUNKS, steps, size, lanes), F32),
            pltpu.VMEM((CHUNKS, tm_count - 1, size, lanes), F32),
            slots,
        ]
        + [pltpu.VMEM((2 * size, 2 * size), BF16)] * 5
        + [square]
        + [pltpu.SemaphoreType.DMA((6 + rows,))]
        + [dma] * 7,
        compiler_params=pltpu.CompilerParams(
            collective_id=0, has_side_effects=True, vmem_limit_bytes=58000 * 1024
        ),
        name="exchange",
    )(
        residual_field,
        eigvec_x,
        eigvec_y,
        eigvec_z,
        eigval_x.reshape(1, -1),
        eigval_y,
        eigval_z.reshape(1, -1),
    )
    return pl.pallas_call(
        inverse_kernel,
        out_shape=jax.ShapeDtypeStruct((steps, rows, size, lanes), F32),
        in_specs=[hbm] * 2,
        out_specs=hbm,
        scratch_shapes=[
            spread,
            square,
            pltpu.VMEM((steps, rows, size, lanes), F32),
            pltpu.VMEM((2 * size, 2 * size), BF16),
            pltpu.SemaphoreType.DMA((rows + 1,)),
            pltpu.SemaphoreType.DMA((rows,)),
        ],
        compiler_params=pltpu.CompilerParams(vmem_limit_bytes=60000 * 1024),
        name="inverse",
    )(turned, eigvec_y)


def solution(mesh):
    placed = (P("tm", "space", None, None), P(), P(), P(), P(), P(), P())
    return jax.shard_map(
        shards, mesh=mesh, in_specs=placed, out_specs=P("tm", "space", None, None), check_vma=False
    )
```

```python
import functools

import jax
import jax.numpy as jnp
from jax import lax
from jax.experimental import pallas as pl
from jax.experimental.pallas import tpu as pltpu
from jax.sharding import PartitionSpec as P

ALPHA = 0.01
CHUNKS = 4
GROUP = 2
LAST_ORDER = (0, 1, 2, 3, 4, 7, 5, 6)
F32 = jnp.float32
BF16 = jnp.bfloat16
MESH = pl.DeviceIdType.MESH


def halves(v):
    high = v.astype(BF16)
    return high, (v - high.astype(F32)).astype(BF16)


def left_weight(w):
    high, low = halves(w)
    return jnp.concatenate(
        [jnp.concatenate([high, high], 1), jnp.concatenate([low, low], 1)], 0
    )


def right_weight(w):
    half = jnp.concatenate(list(halves(w)), 1)
    return jnp.concatenate([half, half], 0)


def left_dot(weight, v):
    rows = v.shape[0]
    out = jnp.dot(weight, jnp.concatenate(list(halves(v)), 0), preferred_element_type=F32)
    return out[:rows] + out[rows:]


def right_dot(v, weight):
    columns = v.shape[1]
    out = jnp.dot(jnp.concatenate(list(halves(v)), 1), weight, preferred_element_type=F32)
    return out[:, :columns] + out[:, columns:]


def stacked(pair):
    columns = pair.shape[1] // 2
    return jnp.concatenate([pair[:, :columns], pair[:, columns:]], 0)


def exchange_kernel(
    field_hbm, vec_x_hbm, vec_y_hbm, vec_z_hbm, val_x_hbm, val_y_hbm, val_z_hbm,
    turned,
    field, vec_x, vec_y, vec_z, val_x, val_y, val_z,
    sent, landed, states, carries, solved, fwd_x, bwd_x, fwd_y, fwd_z, inv_z, decay,
    load, s_send, s_recv, c_send, c_recv, b_send, b_recv, store, heard,
):
    steps, rows, size, lanes = field.shape
    tm_count, space_count = lax.axis_size("tm"), lax.axis_size("space")
    me_t, me = lax.axis_index("tm"), lax.axis_index("space")
    block = size // CHUNKS

    place_x, place_z, core = lax.div(me, 16), lax.rem(lax.div(me, 2), 8), lax.rem(me, 2)
    along_x = [place_x * 16, 16 - place_x * 16]
    along_core = [core, 1 - core]
    partners = []
    for away in (0, 1, -1, 2, -2, 3, -3, 4):
        at_z = lax.rem(place_z + (away + 8), 8) * 2
        for at_x in along_x:
            partners += [at_x + at_z + at_core for at_core in along_core]
    partners = partners[1:]
    followers = [lax.rem(me_t + m, tm_count) for m in range(1, tm_count)]

    loads = [
        pltpu.make_async_copy(source, target, load.at[k])
        for k, (source, target) in enumerate(
            [(vec_y_hbm, vec_y)]
            + [
                (field_hbm.at[pl.ds(2 * pair, 2)], field.at[pl.ds(2 * pair, 2)])
                for pair in range(steps // 2)
            ]
            + [
                (vec_z_hbm, vec_z),
                (vec_x_hbm, vec_x),
                (val_x_hbm, val_x),
                (val_y_hbm, val_y),
                (val_z_hbm, val_z),
            ]
        )
    ]
    for copy in loads:
        copy.start()

    half, line = lax.div(me_t, 4) * 4, lax.rem(me_t, 4)
    next_y, last_y = half + lax.rem(line + 1, 4), half + lax.rem(line + 3, 4)
    other_x = 4 - half + line
    next_z, last_z = partners[3], partners[7]

    barrier = pltpu.get_barrier_semaphore()
    for to in partners[:11]:
        pl.semaphore_signal(barrier, 1, device_id={"space": to}, device_id_type=MESH)
    for to in (next_y, last_y, other_x):
        pl.semaphore_signal(barrier, 1, device_id={"tm": to}, device_id_type=MESH)

    sent_rows = sent.reshape(rows * size * steps, lanes)
    landed_rows = landed.reshape(CHUNKS * size * steps, lanes)
    solved_rows = solved.reshape(CHUNKS * size * steps, lanes)

    loads[0].wait()
    fwd_y[...] = left_weight(vec_y[...].T)
    for pair in range(steps // 2):
        loads[1 + pair].wait()
        for x in range(rows):
            plane = jnp.concatenate([field[2 * pair + k, x] for k in range(2)], 1)
            plane = left_dot(fwd_y[...], plane)
            for k in range(2):
                at = pl.ds(x * size * steps + 2 * pair + k, size, stride=steps)
                sent_rows[at, :] = plane[:, k * lanes : (k + 1) * lanes]
    def send(c, to):
        pltpu.make_async_remote_copy(
            sent.at[:, c * block + to],
            landed.at[c, pl.ds(rows * me, rows)],
            s_send.at[c],
            s_recv.at[c],
            device_id={"space": to},
            device_id_type=MESH,
        ).start()

    def tell(axis, to, news):
        pl.semaphore_signal(heard.at[news], 1, device_id={axis: to}, device_id_type=MESH)

    def hear(news):
        pl.semaphore_wait(heard.at[news], 1)

    pl.semaphore_wait(barrier, 14)
    tell("space", last_z, 0)
    tell("space", next_z, 1)
    tell("tm", last_y, 5)
    tell("tm", other_x, 6)
    for to in partners[:11]:
        send(0, to)
    hear(0)
    tell("space", last_z, 2)
    hear(1)
    tell("space", next_z, 3)
    for to in partners[11:19]:
        send(0, to)
    hear(2)
    tell("space", last_z, 4)
    hear(3)
    for to in partners[19:27]:
        send(0, to)
    hear(4)
    for to in partners[27:]:
        send(0, to)

    @pl.loop(1, CHUNKS)
    def _(c):
        for to in partners:
            send(c, to)

    hear(5)
    tell("tm", other_x, 7)
    hear(6)
    hear(7)

    for copy in loads[1 + steps // 2 :]:
        copy.wait()
    fwd_z[...] = right_weight(vec_z[...])
    fwd_x[...] = left_weight(vec_x[...].T)
    bwd_x[...] = left_weight(vec_x[...])
    inv_z[...] = right_weight(vec_z[...].T)
    column_x = jnp.broadcast_to(val_x[...], (size, lanes)).T

    def whole(c):
        return landed.at[c, pl.ds(0, size - rows)]

    def own_block(c):
        return pltpu.make_async_copy(
            solved.at[c, pl.ds(rows * me, rows)], turned.at[:, c * block + me], store.at[c]
        )

    def whole_back(c):
        return turned.at[:, pl.ds(c * block, block - 1)]

    @pl.loop(0, CHUNKS)
    def _(c):
        landed[c, pl.ds(rows * me, rows)] = sent[:, c * block + me]
        shift = column_x + (val_y[c * block + me] + val_z[...])
        decay[...] = 1.0 / (1.0 + shift)
        pltpu.make_async_copy(whole(c), whole(c), s_recv.at[c]).wait()
        state = jnp.zeros((size, lanes), F32)
        for pair in range(steps // 2):
            first = c * size * steps + 2 * pair
            plane = jnp.concatenate(
                [landed_rows[pl.ds(first + k, size, stride=steps), :] for k in range(2)], 1
            )
            plane = stacked(left_dot(fwd_x[...], plane))
            plane = right_dot(plane, fwd_z[...])
            for k in range(2):
                state = decay[...] * (plane[k * size : (k + 1) * size] + state)
                states[c, 2 * pair + k] = state

        for m, to in enumerate(followers):
            pltpu.make_async_remote_copy(
                states.at[c, steps - 1],
                carries.at[c, m],
                c_send.at[c],
                c_recv.at[c],
                device_id={"tm": to},
                device_id_type=MESH,
            ).start()

        pltpu.make_async_copy(carries.at[c], carries.at[c], c_recv.at[c]).wait()
        a = decay[...]
        a8 = a
        for _ in range(3):
            a8 = a8 * a8
        whole_decay = a8
        for _ in range(3):
            whole_decay = whole_decay * whole_decay
        total = ALPHA * states[c, steps - 1]
        for m in range(tm_count - 1, 0, -1):
            weight = jnp.where(me_t < m, ALPHA, 1.0).astype(F32)
            total = total * a8 + weight * carries[c, m - 1]
        past = a * (total / (1.0 - ALPHA * whole_decay))
        for pair in range(steps // 2):
            planes = []
            for k in range(2):
                planes.append(states[c, 2 * pair + k] + past)
                past = past * a
            plane = stacked(left_dot(bwd_x[...], jnp.concatenate(planes, 1)))
            plane = right_dot(plane, inv_z[...])
            for k in range(2):
                at = pl.ds(c * size * steps + 2 * pair + k, size, stride=steps)
                solved_rows[at, :] = plane[k * size : (k + 1) * size]

        def send_back(to):
            pltpu.make_async_remote_copy(
                solved.at[c, pl.ds(rows * to, rows)],
                turned.at[:, c * block + me],
                b_send.at[c],
                b_recv.at[c],
                device_id={"space": to},
                device_id_type=MESH,
            ).start()

        @pl.when(c < CHUNKS - 1)
        def _():
            for to in partners:
                send_back(to)

        @pl.when(c == CHUNKS - 1)
        def _():
            for at_z in LAST_ORDER:
                for at_x in along_x:
                    for at_core in along_core:
                        to = at_x + 2 * at_z + at_core
                        if at_x is along_x[0] and at_core is along_core[0]:
                            pl.when(place_z != at_z)(functools.partial(send_back, to))
                        else:
                            send_back(to)

        own_block(c).start()

    @pl.loop(0, CHUNKS)
    def _(c):
        own_block(c).wait()
        pltpu.make_async_copy(whole(c), whole(c), s_send.at[c]).wait()
        pltpu.make_async_copy(carries.at[c], carries.at[c], c_send.at[c]).wait()
        pltpu.make_async_copy(whole_back(c), whole_back(c), b_recv.at[c]).wait()
        pltpu.make_async_copy(whole(c), whole(c), b_send.at[c]).wait()


def inverse_kernel(turned_hbm, vec_y_hbm, update_hbm, turned, vec_y, update, inv_y, load, store):
    count, size, steps, lanes = turned.shape
    loads = [pltpu.make_async_copy(vec_y_hbm, vec_y, load.at[count])] + [
        pltpu.make_async_copy(turned_hbm.at[x], turned.at[x], load.at[x]) for x in range(count)
    ]
    for copy in loads:
        copy.start()
    loads[0].wait()
    inv_y[...] = left_weight(vec_y[...])
    rows = turned.reshape(count * size * steps, lanes)
    stores = []
    for group in range(0, count, GROUP):
        for copy in loads[1 + group : 1 + group + GROUP]:
            copy.wait()
        for x in range(group, group + GROUP):
            for pair in range(steps // 2):
                first = x * size * steps + 2 * pair
                plane = jnp.concatenate(
                    [rows[pl.ds(first + k, size, stride=steps), :] for k in range(2)], 1
                )
                plane = left_dot(inv_y[...], plane)
                for k in range(2):
                    update[2 * pair + k, x] = plane[:, k * lanes : (k + 1) * lanes]
        for x in range(group, group + GROUP):
            part = update_hbm.at[:, x]
            stores.append(pltpu.make_async_copy(update.at[:, x], part, store.at[x]))
            stores[-1].start()
    for copy in stores:
        copy.wait()


def shards(residual_field, eigvec_x, eigvec_y, eigvec_z, eigval_x, eigval_y, eigval_z):
    steps, rows, size, lanes = residual_field.shape
    tm_count = lax.axis_size("tm")
    hbm = pl.BlockSpec(memory_space=pltpu.HBM)
    square = pltpu.VMEM((size, size), F32)
    spread = pltpu.VMEM((rows, size, steps, lanes), F32)
    slots = pltpu.VMEM((CHUNKS, size, steps, lanes), F32)
    dma = pltpu.SemaphoreType.DMA((CHUNKS,))
    turned = pl.pallas_call(
        exchange_kernel,
        out_shape=jax.ShapeDtypeStruct((rows, size, steps, lanes), F32),
        in_specs=[hbm] * 7,
        out_specs=hbm,
        scratch_shapes=[
            pltpu.VMEM((steps, rows, size, lanes), F32),
            square,
            square,
            square,
            pltpu.VMEM((1, lanes), F32),
            pltpu.SMEM((size,), F32),
            pltpu.VMEM((1, lanes), F32),
            spread,
            slots,
            pltpu.VMEM((CHUNKS, steps, size, lanes), F32),
            pltpu.VMEM((CHUNKS, tm_count - 1, size, lanes), F32),
            slots,
        ]
        + [pltpu.VMEM((2 * size, 2 * size), BF16)] * 5
        + [square]
        + [pltpu.SemaphoreType.DMA((6 + steps // 2,))]
        + [dma] * 7
        + [pltpu.SemaphoreType.REGULAR((8,))],
        compiler_params=pltpu.CompilerParams(
            collective_id=0, has_side_effects=True, vmem_limit_bytes=58000 * 1024
        ),
        name="exchange",
    )(
        residual_field,
        eigvec_x,
        eigvec_y,
        eigvec_z,
        eigval_x.reshape(1, -1),
        eigval_y,
        eigval_z.reshape(1, -1),
    )
    return pl.pallas_call(
        inverse_kernel,
        out_shape=jax.ShapeDtypeStruct((steps, rows, size, lanes), F32),
        in_specs=[hbm] * 2,
        out_specs=hbm,
        scratch_shapes=[
            spread,
            square,
            pltpu.VMEM((steps, rows, size, lanes), F32),
            pltpu.VMEM((2 * size, 2 * size), BF16),
            pltpu.SemaphoreType.DMA((rows + 1,)),
            pltpu.SemaphoreType.DMA((rows,)),
        ],
        compiler_params=pltpu.CompilerParams(vmem_limit_bytes=60000 * 1024),
        name="inverse",
    )(turned, eigvec_y)


def solution(mesh):
    placed = (P("tm", "space", None, None), P(), P(), P(), P(), P(), P())
    return jax.shard_map(
        shards, mesh=mesh, in_specs=placed, out_specs=P("tm", "space", None, None), check_vma=False
    )
```

```python
import functools

import jax
import jax.numpy as jnp
from jax import lax
from jax.experimental import pallas as pl
from jax.experimental.pallas import tpu as pltpu
from jax.sharding import PartitionSpec as P

ALPHA = 0.01
CHUNKS = 4
GROUP = 2
LAST_ORDER = (0, 1, 2, 3, 4, 7, 5, 6)
F32 = jnp.float32
BF16 = jnp.bfloat16
MESH = pl.DeviceIdType.MESH


def halves(v):
    high = v.astype(BF16)
    return high, (v - high.astype(F32)).astype(BF16)


def left_weight(w):
    high, low = halves(w)
    return jnp.concatenate(
        [jnp.concatenate([high, high], 1), jnp.concatenate([low, low], 1)], 0
    )


def right_weight(w):
    half = jnp.concatenate(list(halves(w)), 1)
    return jnp.concatenate([half, half], 0)


def left_dot(weight, v):
    rows = weight.shape[0] // 2
    out = jnp.dot(weight, jnp.concatenate(list(halves(v)), 0), preferred_element_type=F32)
    return out[:rows] + out[rows:]


def right_dot(v, weight):
    columns = v.shape[1]
    out = jnp.dot(jnp.concatenate(list(halves(v)), 1), weight, preferred_element_type=F32)
    return out[:, :columns] + out[:, columns:]


def stacked(pair):
    columns = pair.shape[1] // 2
    return jnp.concatenate([pair[:, :columns], pair[:, columns:]], 0)


def exchange_kernel(
    field_hbm, vec_x_hbm, vec_y_hbm, vec_z_hbm, val_x_hbm, val_y_hbm, val_z_hbm,
    turned,
    field, vec_x, vec_y, vec_z, val_x, val_y, val_z,
    sent, landed, states, carries, solved, first_y, fwd_y, fwd_x, bwd_x, fwd_z, inv_z, decay,
    load, s_send, s_recv, c_send, c_recv, b_send, b_recv, store, heard,
):
    steps, rows, size, lanes = field.shape
    tm_count, space_count = lax.axis_size("tm"), lax.axis_size("space")
    me_t, me = lax.axis_index("tm"), lax.axis_index("space")
    block = size // CHUNKS

    place_x, place_z, core = lax.div(me, 16), lax.rem(lax.div(me, 2), 8), lax.rem(me, 2)
    along_x = [place_x * 16, 16 - place_x * 16]
    along_core = [core, 1 - core]
    partners = []
    for away in (0, 1, -1, 2, -2, 3, -3, 4):
        at_z = lax.rem(place_z + (away + 8), 8) * 2
        for at_x in along_x:
            partners += [at_x + at_z + at_core for at_core in along_core]
    partners = partners[1:]
    followers = [lax.rem(me_t + m, tm_count) for m in range(1, tm_count)]

    loads = [
        pltpu.make_async_copy(source, target, load.at[k])
        for k, (source, target) in enumerate(
            [(vec_y_hbm, vec_y)]
            + [
                (field_hbm.at[pl.ds(2 * pair, 2)], field.at[pl.ds(2 * pair, 2)])
                for pair in range(steps // 2)
            ]
            + [
                (vec_z_hbm, vec_z),
                (vec_x_hbm, vec_x),
                (val_x_hbm, val_x),
                (val_y_hbm, val_y),
                (val_z_hbm, val_z),
            ]
        )
    ]
    for copy in loads:
        copy.start()

    half, line = lax.div(me_t, 4) * 4, lax.rem(me_t, 4)
    next_y, last_y = half + lax.rem(line + 1, 4), half + lax.rem(line + 3, 4)
    other_x = 4 - half + line
    next_z, last_z = partners[3], partners[7]

    barrier = pltpu.get_barrier_semaphore()
    for to in partners[:11]:
        pl.semaphore_signal(barrier, 1, device_id={"space": to}, device_id_type=MESH)
    for to in (next_y, last_y, other_x):
        pl.semaphore_signal(barrier, 1, device_id={"tm": to}, device_id_type=MESH)

    sent_rows = sent.reshape(rows * size * steps, lanes)
    landed_rows = landed.reshape(CHUNKS * size * steps, lanes)
    solved_rows = solved.reshape(CHUNKS * size * steps, lanes)

    def forward_y(weight, start, pair, x):
        plane = jnp.concatenate([field[2 * pair + k, x] for k in range(2)], 1)
        plane = left_dot(weight[...], plane)
        for k in range(2):
            first = (x * size + start) * steps + 2 * pair + k
            at = pl.ds(first, plane.shape[0], stride=steps)
            sent_rows[at, :] = plane[:, k * lanes : (k + 1) * lanes]

    loads[0].wait()
    turned_y = vec_y[...].T
    first_y[...] = left_weight(turned_y[:block])
    fwd_y[...] = left_weight(turned_y[block:])
    for pair in range(steps // 2):
        loads[1 + pair].wait()
        for x in range(rows):
            forward_y(first_y, 0, pair, x)

    def send(c, to):
        pltpu.make_async_remote_copy(
            sent.at[:, c * block + to],
            landed.at[c, pl.ds(rows * me, rows)],
            s_send.at[c],
            s_recv.at[c],
            device_id={"space": to},
            device_id_type=MESH,
        ).start()

    def tell(axis, to, news):
        pl.semaphore_signal(heard.at[news], 1, device_id={axis: to}, device_id_type=MESH)

    def hear(news):
        pl.semaphore_wait(heard.at[news], 1)

    pl.semaphore_wait(barrier, 14)
    tell("space", last_z, 0)
    tell("space", next_z, 1)
    tell("tm", last_y, 5)
    tell("tm", other_x, 6)
    for to in partners[:11]:
        send(0, to)
    hear(0)
    tell("space", last_z, 2)
    hear(1)
    tell("space", next_z, 3)
    for to in partners[11:19]:
        send(0, to)
    hear(2)
    tell("space", last_z, 4)
    hear(3)
    for to in partners[19:27]:
        send(0, to)
    hear(4)
    for to in partners[27:]:
        send(0, to)

    @pl.loop(0, steps // 2)
    def _(pair):
        for x in range(rows):
            forward_y(fwd_y, block, pair, x)

    @pl.loop(1, CHUNKS)
    def _(c):
        for to in partners:
            send(c, to)

    hear(5)
    tell("tm", other_x, 7)
    hear(6)
    hear(7)

    for copy in loads[1 + steps // 2 :]:
        copy.wait()
    fwd_z[...] = right_weight(vec_z[...])
    fwd_x[...] = left_weight(vec_x[...].T)
    bwd_x[...] = left_weight(vec_x[...])
    inv_z[...] = right_weight(vec_z[...].T)
    column_x = jnp.broadcast_to(val_x[...], (size, lanes)).T

    def whole(c):
        return landed.at[c, pl.ds(0, size - rows)]

    def own_block(c):
        return pltpu.make_async_copy(
            solved.at[c, pl.ds(rows * me, rows)], turned.at[:, c * block + me], store.at[c]
        )

    def whole_back(c):
        return turned.at[:, pl.ds(c * block, block - 1)]

    @pl.loop(0, CHUNKS)
    def _(c):
        landed[c, pl.ds(rows * me, rows)] = sent[:, c * block + me]
        shift = column_x + (val_y[c * block + me] + val_z[...])
        decay[...] = 1.0 / (1.0 + shift)
        pltpu.make_async_copy(whole(c), whole(c), s_recv.at[c]).wait()
        state = jnp.zeros((size, lanes), F32)
        for pair in range(steps // 2):
            first = c * size * steps + 2 * pair
            plane = jnp.concatenate(
                [landed_rows[pl.ds(first + k, size, stride=steps), :] for k in range(2)], 1
            )
            plane = stacked(left_dot(fwd_x[...], plane))
            plane = right_dot(plane, fwd_z[...])
            for k in range(2):
                state = decay[...] * (plane[k * size : (k + 1) * size] + state)
                states[c, 2 * pair + k] = state

        for m, to in enumerate(followers):
            pltpu.make_async_remote_copy(
                states.at[c, steps - 1],
                carries.at[c, m],
                c_send.at[c],
                c_recv.at[c],
                device_id={"tm": to},
                device_id_type=MESH,
            ).start()

        pltpu.make_async_copy(carries.at[c], carries.at[c], c_recv.at[c]).wait()
        a = decay[...]
        a8 = a
        for _ in range(3):
            a8 = a8 * a8
        whole_decay = a8
        for _ in range(3):
            whole_decay = whole_decay * whole_decay
        total = ALPHA * states[c, steps - 1]
        for m in range(tm_count - 1, 0, -1):
            weight = jnp.where(me_t < m, ALPHA, 1.0).astype(F32)
            total = total * a8 + weight * carries[c, m - 1]
        past = a * (total / (1.0 - ALPHA * whole_decay))
        for pair in range(steps // 2):
            planes = []
            for k in range(2):
                planes.append(states[c, 2 * pair + k] + past)
                past = past * a
            plane = stacked(left_dot(bwd_x[...], jnp.concatenate(planes, 1)))
            plane = right_dot(plane, inv_z[...])
            for k in range(2):
                at = pl.ds(c * size * steps + 2 * pair + k, size, stride=steps)
                solved_rows[at, :] = plane[k * size : (k + 1) * size]

        def send_back(to):
            pltpu.make_async_remote_copy(
                solved.at[c, pl.ds(rows * to, rows)],
                turned.at[:, c * block + me],
                b_send.at[c],
                b_recv.at[c],
                device_id={"space": to},
                device_id_type=MESH,
            ).start()

        @pl.when(c < CHUNKS - 1)
        def _():
            for to in partners:
                send_back(to)

        @pl.when(c == CHUNKS - 1)
        def _():
            for at_z in LAST_ORDER:
                for at_x in along_x:
                    for at_core in along_core:
                        to = at_x + 2 * at_z + at_core
                        if at_x is along_x[0] and at_core is along_core[0]:
                            pl.when(place_z != at_z)(functools.partial(send_back, to))
                        else:
                            send_back(to)

        own_block(c).start()

    @pl.loop(0, CHUNKS)
    def _(c):
        own_block(c).wait()
        pltpu.make_async_copy(whole(c), whole(c), s_send.at[c]).wait()
        pltpu.make_async_copy(carries.at[c], carries.at[c], c_send.at[c]).wait()
        pltpu.make_async_copy(whole_back(c), whole_back(c), b_recv.at[c]).wait()
        pltpu.make_async_copy(whole(c), whole(c), b_send.at[c]).wait()


def inverse_kernel(turned_hbm, vec_y_hbm, update_hbm, turned, vec_y, update, inv_y, load, store):
    count, size, steps, lanes = turned.shape
    loads = [pltpu.make_async_copy(vec_y_hbm, vec_y, load.at[count])] + [
        pltpu.make_async_copy(turned_hbm.at[x], turned.at[x], load.at[x]) for x in range(count)
    ]
    for copy in loads:
        copy.start()
    loads[0].wait()
    inv_y[...] = left_weight(vec_y[...])
    rows = turned.reshape(count * size * steps, lanes)
    stores = []
    for group in range(0, count, GROUP):
        for copy in loads[1 + group : 1 + group + GROUP]:
            copy.wait()
        for x in range(group, group + GROUP):
            for pair in range(steps // 2):
                first = x * size * steps + 2 * pair
                plane = jnp.concatenate(
                    [rows[pl.ds(first + k, size, stride=steps), :] for k in range(2)], 1
                )
                plane = left_dot(inv_y[...], plane)
                for k in range(2):
                    update[2 * pair + k, x] = plane[:, k * lanes : (k + 1) * lanes]
        for x in range(group, group + GROUP):
            part = update_hbm.at[:, x]
            stores.append(pltpu.make_async_copy(update.at[:, x], part, store.at[x]))
            stores[-1].start()
    for copy in stores:
        copy.wait()


def shards(residual_field, eigvec_x, eigvec_y, eigvec_z, eigval_x, eigval_y, eigval_z):
    steps, rows, size, lanes = residual_field.shape
    tm_count = lax.axis_size("tm")
    hbm = pl.BlockSpec(memory_space=pltpu.HBM)
    square = pltpu.VMEM((size, size), F32)
    spread = pltpu.VMEM((rows, size, steps, lanes), F32)
    slots = pltpu.VMEM((CHUNKS, size, steps, lanes), F32)
    dma = pltpu.SemaphoreType.DMA((CHUNKS,))
    turned = pl.pallas_call(
        exchange_kernel,
        out_shape=jax.ShapeDtypeStruct((rows, size, steps, lanes), F32),
        in_specs=[hbm] * 7,
        out_specs=hbm,
        scratch_shapes=[
            pltpu.VMEM((steps, rows, size, lanes), F32),
            square,
            square,
            square,
            pltpu.VMEM((1, lanes), F32),
            pltpu.SMEM((size,), F32),
            pltpu.VMEM((1, lanes), F32),
            spread,
            slots,
            pltpu.VMEM((CHUNKS, steps, size, lanes), F32),
            pltpu.VMEM((CHUNKS, tm_count - 1, size, lanes), F32),
            slots,
            pltpu.VMEM((2 * size // CHUNKS, 2 * size), BF16),
            pltpu.VMEM((2 * size - 2 * size // CHUNKS, 2 * size), BF16),
        ]
        + [pltpu.VMEM((2 * size, 2 * size), BF16)] * 4
        + [square]
        + [pltpu.SemaphoreType.DMA((6 + steps // 2,))]
        + [dma] * 7
        + [pltpu.SemaphoreType.REGULAR((8,))],
        compiler_params=pltpu.CompilerParams(
            collective_id=0, has_side_effects=True, vmem_limit_bytes=58000 * 1024
        ),
        name="exchange",
    )(
        residual_field,
        eigvec_x,
        eigvec_y,
        eigvec_z,
        eigval_x.reshape(1, -1),
        eigval_y,
        eigval_z.reshape(1, -1),
    )
    return pl.pallas_call(
        inverse_kernel,
        out_shape=jax.ShapeDtypeStruct((steps, rows, size, lanes), F32),
        in_specs=[hbm] * 2,
        out_specs=hbm,
        scratch_shapes=[
            spread,
            square,
            pltpu.VMEM((steps, rows, size, lanes), F32),
            pltpu.VMEM((2 * size, 2 * size), BF16),
            pltpu.SemaphoreType.DMA((rows + 1,)),
            pltpu.SemaphoreType.DMA((rows,)),
        ],
        compiler_params=pltpu.CompilerParams(vmem_limit_bytes=60000 * 1024),
        name="inverse",
    )(turned, eigvec_y)


def solution(mesh):
    placed = (P("tm", "space", None, None), P(), P(), P(), P(), P(), P())
    return jax.shard_map(
        shards, mesh=mesh, in_specs=placed, out_specs=P("tm", "space", None, None), check_vma=False
    )
```

```python
import functools

import jax
import jax.numpy as jnp
from jax import lax
from jax.experimental import pallas as pl
from jax.experimental.pallas import tpu as pltpu
from jax.sharding import PartitionSpec as P

ALPHA = 0.01
CHUNKS = 4
GROUP = 2
LAST_ORDER = (0, 1, 2, 3, 4, 7, 5, 6)
F32 = jnp.float32
BF16 = jnp.bfloat16
MESH = pl.DeviceIdType.MESH


def halves(v):
    high = v.astype(BF16)
    return high, (v - high.astype(F32)).astype(BF16)


def left_weight(w):
    high, low = halves(w)
    return jnp.concatenate(
        [jnp.concatenate([high, high], 1), jnp.concatenate([low, low], 1)], 0
    )


def right_weight(w):
    half = jnp.concatenate(list(halves(w)), 1)
    return jnp.concatenate([half, half], 0)


def left_dot(weight, v):
    rows = weight.shape[0] // 2
    out = jnp.dot(weight, jnp.concatenate(list(halves(v)), 0), preferred_element_type=F32)
    return out[:rows] + out[rows:]


def right_dot(v, weight):
    columns = v.shape[1]
    out = jnp.dot(jnp.concatenate(list(halves(v)), 1), weight, preferred_element_type=F32)
    return out[:, :columns] + out[:, columns:]


def stacked(pair):
    columns = pair.shape[1] // 2
    return jnp.concatenate([pair[:, :columns], pair[:, columns:]], 0)


def exchange_kernel(
    field_hbm, vec_x_hbm, vec_y_hbm, vec_z_hbm, val_x_hbm, val_y_hbm, val_z_hbm,
    turned,
    field, vec_x, vec_y, vec_z, val_x, val_y, val_z,
    sent, landed, states, carries, solved, first_y, fwd_y, fwd_x, bwd_x, fwd_z, inv_z, decay,
    load, s_send, s_recv, c_send, c_recv, b_send, b_recv, store, heard,
):
    steps, rows, size, lanes = field.shape
    tm_count, space_count = lax.axis_size("tm"), lax.axis_size("space")
    me_t, me = lax.axis_index("tm"), lax.axis_index("space")
    block = size // CHUNKS

    place_x, place_z, core = lax.div(me, 16), lax.rem(lax.div(me, 2), 8), lax.rem(me, 2)
    along_x = [place_x * 16, 16 - place_x * 16]
    along_core = [core, 1 - core]
    partners = []
    for away in (0, 1, -1, 2, -2, 3, -3, 4):
        at_z = lax.rem(place_z + (away + 8), 8) * 2
        for at_x in along_x:
            partners += [at_x + at_z + at_core for at_core in along_core]
    partners = partners[1:]
    followers = [lax.rem(me_t + m, tm_count) for m in range(1, tm_count)]

    loads = [
        pltpu.make_async_copy(source, target, load.at[k])
        for k, (source, target) in enumerate(
            [(vec_y_hbm, vec_y)]
            + [
                (field_hbm.at[pl.ds(2 * pair, 2)], field.at[pl.ds(2 * pair, 2)])
                for pair in range(steps // 2)
            ]
            + [
                (vec_z_hbm, vec_z),
                (vec_x_hbm, vec_x),
                (val_x_hbm, val_x),
                (val_y_hbm, val_y),
                (val_z_hbm, val_z),
            ]
        )
    ]
    for copy in loads:
        copy.start()

    half, line = lax.div(me_t, 4) * 4, lax.rem(me_t, 4)
    next_y, last_y = half + lax.rem(line + 1, 4), half + lax.rem(line + 3, 4)
    other_x = 4 - half + line
    next_z, last_z = partners[3], partners[7]

    barrier = pltpu.get_barrier_semaphore()
    for to in partners[:11]:
        pl.semaphore_signal(barrier, 1, device_id={"space": to}, device_id_type=MESH)
    for to in (next_y, last_y, other_x):
        pl.semaphore_signal(barrier, 1, device_id={"tm": to}, device_id_type=MESH)

    sent_rows = sent.reshape(rows * size * steps, lanes)
    landed_rows = landed.reshape(CHUNKS * size * steps, lanes)
    solved_rows = solved.reshape(CHUNKS * size * steps, lanes)

    def forward_y(weight, start, pair, x):
        plane = jnp.concatenate([field[2 * pair + k, x] for k in range(2)], 1)
        plane = left_dot(weight[...], plane)
        for k in range(2):
            first = (x * size + start) * steps + 2 * pair + k
            at = pl.ds(first, plane.shape[0], stride=steps)
            sent_rows[at, :] = plane[:, k * lanes : (k + 1) * lanes]

    loads[0].wait()
    turned_y = vec_y[...].T
    first_y[...] = left_weight(turned_y[:block])
    fwd_y[...] = left_weight(turned_y[block:])
    for pair in range(steps // 2):
        loads[1 + pair].wait()
        for x in range(rows):
            forward_y(first_y, 0, pair, x)

    def send(c, to):
        pltpu.make_async_remote_copy(
            sent.at[:, c * block + to],
            landed.at[c, pl.ds(rows * me, rows)],
            s_send.at[c],
            s_recv.at[c],
            device_id={"space": to},
            device_id_type=MESH,
        ).start()

    def tell(axis, to, news):
        pl.semaphore_signal(heard.at[news], 1, device_id={axis: to}, device_id_type=MESH)

    def hear(news):
        pl.semaphore_wait(heard.at[news], 1)

    pl.semaphore_wait(barrier, 14)
    tell("space", last_z, 0)
    tell("space", next_z, 1)
    tell("tm", last_y, 5)
    tell("tm", other_x, 6)
    for to in partners[:11]:
        send(0, to)
    hear(0)
    tell("space", last_z, 2)
    hear(1)
    tell("space", next_z, 3)
    for to in partners[11:19]:
        send(0, to)
    hear(2)
    tell("space", last_z, 4)
    hear(3)
    for to in partners[19:27]:
        send(0, to)
    hear(4)
    for to in partners[27:]:
        send(0, to)

    @pl.loop(0, steps // 2)
    def _(pair):
        for x in range(rows):
            forward_y(fwd_y, block, pair, x)

    @pl.loop(1, CHUNKS)
    def _(c):
        for to in partners:
            send(c, to)

    hear(5)
    tell("tm", other_x, 7)
    hear(6)
    hear(7)

    for copy in loads[1 + steps // 2 :]:
        copy.wait()
    fwd_z[...] = right_weight(vec_z[...])
    fwd_x[...] = left_weight(vec_x[...].T)
    bwd_x[...] = left_weight(vec_x[...])
    inv_z[...] = right_weight(vec_z[...].T)
    column_x = jnp.broadcast_to(val_x[...], (size, lanes)).T

    def whole(c):
        return landed.at[c, pl.ds(0, size - rows)]

    def own_block(c):
        return pltpu.make_async_copy(
            solved.at[c, pl.ds(rows * me, rows)], turned.at[:, c * block + me], store.at[c]
        )

    def whole_back(c):
        return turned.at[:, pl.ds(c * block, block - 1)]

    @pl.loop(0, CHUNKS)
    def _(c):
        landed[c, pl.ds(rows * me, rows)] = sent[:, c * block + me]
        shift = column_x + (val_y[c * block + me] + val_z[...])
        decay[...] = 1.0 / (1.0 + shift)
        pltpu.make_async_copy(whole(c), whole(c), s_recv.at[c]).wait()
        state = jnp.zeros((size, lanes), F32)
        for pair in range(steps // 2):
            first = c * size * steps + 2 * pair
            plane = jnp.concatenate(
                [landed_rows[pl.ds(first + k, size, stride=steps), :] for k in range(2)], 1
            )
            plane = stacked(left_dot(fwd_x[...], plane))
            plane = right_dot(plane, fwd_z[...])
            for k in range(2):
                state = decay[...] * (plane[k * size : (k + 1) * size] + state)
                states[c, 2 * pair + k] = state

        for m, to in enumerate(followers):
            pltpu.make_async_remote_copy(
                states.at[c, steps - 1],
                carries.at[c, m],
                c_send.at[c],
                c_recv.at[c],
                device_id={"tm": to},
                device_id_type=MESH,
            ).start()

        pltpu.make_async_copy(carries.at[c], carries.at[c], c_recv.at[c]).wait()
        a = decay[...]
        a8 = a
        for _ in range(3):
            a8 = a8 * a8
        whole_decay = a8
        for _ in range(3):
            whole_decay = whole_decay * whole_decay
        total = ALPHA * states[c, steps - 1]
        for m in range(tm_count - 1, 0, -1):
            weight = jnp.where(me_t < m, ALPHA, 1.0).astype(F32)
            total = total * a8 + weight * carries[c, m - 1]
        past = a * (total / (1.0 - ALPHA * whole_decay))
        for pair in range(steps // 2):
            planes = []
            for k in range(2):
                planes.append(states[c, 2 * pair + k] + past)
                past = past * a
            plane = stacked(left_dot(bwd_x[...], jnp.concatenate(planes, 1)))
            plane = right_dot(plane, inv_z[...])
            for k in range(2):
                at = pl.ds(c * size * steps + 2 * pair + k, size, stride=steps)
                solved_rows[at, :] = plane[k * size : (k + 1) * size]

        def send_back(to):
            pltpu.make_async_remote_copy(
                solved.at[c, pl.ds(rows * to, rows)],
                turned.at[:, c * block + me],
                b_send.at[c],
                b_recv.at[c],
                device_id={"space": to},
                device_id_type=MESH,
            ).start()

        @pl.when(c < CHUNKS - 1)
        def _():
            for to in partners:
                send_back(to)

        @pl.when(c == CHUNKS - 1)
        def _():
            for at_z in LAST_ORDER:
                for at_x in along_x:
                    for at_core in (1, 0):
                        to = at_x + 2 * at_z + at_core
                        if at_x is along_x[0]:
                            pl.when(to != me)(functools.partial(send_back, to))
                        else:
                            send_back(to)

        own_block(c).start()

    @pl.loop(0, CHUNKS)
    def _(c):
        own_block(c).wait()
        pltpu.make_async_copy(whole(c), whole(c), s_send.at[c]).wait()
        pltpu.make_async_copy(carries.at[c], carries.at[c], c_send.at[c]).wait()
        pltpu.make_async_copy(whole_back(c), whole_back(c), b_recv.at[c]).wait()
        pltpu.make_async_copy(whole(c), whole(c), b_send.at[c]).wait()


def inverse_kernel(turned_hbm, vec_y_hbm, update_hbm, turned, vec_y, update, inv_y, load, store):
    count, size, steps, lanes = turned.shape
    loads = [pltpu.make_async_copy(vec_y_hbm, vec_y, load.at[count])] + [
        pltpu.make_async_copy(turned_hbm.at[x], turned.at[x], load.at[x]) for x in range(count)
    ]
    for copy in loads:
        copy.start()
    loads[0].wait()
    inv_y[...] = left_weight(vec_y[...])
    rows = turned.reshape(count * size * steps, lanes)
    stores = []
    for group in range(0, count, GROUP):
        for copy in loads[1 + group : 1 + group + GROUP]:
            copy.wait()
        for x in range(group, group + GROUP):
            for pair in range(steps // 2):
                first = x * size * steps + 2 * pair
                plane = jnp.concatenate(
                    [rows[pl.ds(first + k, size, stride=steps), :] for k in range(2)], 1
                )
                plane = left_dot(inv_y[...], plane)
                for k in range(2):
                    update[2 * pair + k, x] = plane[:, k * lanes : (k + 1) * lanes]
        for x in range(group, group + GROUP):
            part = update_hbm.at[:, x]
            stores.append(pltpu.make_async_copy(update.at[:, x], part, store.at[x]))
            stores[-1].start()
    for copy in stores:
        copy.wait()


def shards(residual_field, eigvec_x, eigvec_y, eigvec_z, eigval_x, eigval_y, eigval_z):
    steps, rows, size, lanes = residual_field.shape
    tm_count = lax.axis_size("tm")
    hbm = pl.BlockSpec(memory_space=pltpu.HBM)
    square = pltpu.VMEM((size, size), F32)
    spread = pltpu.VMEM((rows, size, steps, lanes), F32)
    slots = pltpu.VMEM((CHUNKS, size, steps, lanes), F32)
    dma = pltpu.SemaphoreType.DMA((CHUNKS,))
    turned = pl.pallas_call(
        exchange_kernel,
        out_shape=jax.ShapeDtypeStruct((rows, size, steps, lanes), F32),
        in_specs=[hbm] * 7,
        out_specs=hbm,
        scratch_shapes=[
            pltpu.VMEM((steps, rows, size, lanes), F32),
            square,
            square,
            square,
            pltpu.VMEM((1, lanes), F32),
            pltpu.SMEM((size,), F32),
            pltpu.VMEM((1, lanes), F32),
            spread,
            slots,
            pltpu.VMEM((CHUNKS, steps, size, lanes), F32),
            pltpu.VMEM((CHUNKS, tm_count - 1, size, lanes), F32),
            slots,
            pltpu.VMEM((2 * size // CHUNKS, 2 * size), BF16),
            pltpu.VMEM((2 * size - 2 * size // CHUNKS, 2 * size), BF16),
        ]
        + [pltpu.VMEM((2 * size, 2 * size), BF16)] * 4
        + [square]
        + [pltpu.SemaphoreType.DMA((6 + steps // 2,))]
        + [dma] * 7
        + [pltpu.SemaphoreType.REGULAR((8,))],
        compiler_params=pltpu.CompilerParams(
            collective_id=0, has_side_effects=True, vmem_limit_bytes=58000 * 1024
        ),
        name="exchange",
    )(
        residual_field,
        eigvec_x,
        eigvec_y,
        eigvec_z,
        eigval_x.reshape(1, -1),
        eigval_y,
        eigval_z.reshape(1, -1),
    )
    return pl.pallas_call(
        inverse_kernel,
        out_shape=jax.ShapeDtypeStruct((steps, rows, size, lanes), F32),
        in_specs=[hbm] * 2,
        out_specs=hbm,
        scratch_shapes=[
            spread,
            square,
            pltpu.VMEM((steps, rows, size, lanes), F32),
            pltpu.VMEM((2 * size, 2 * size), BF16),
            pltpu.SemaphoreType.DMA((rows + 1,)),
            pltpu.SemaphoreType.DMA((rows,)),
        ],
        compiler_params=pltpu.CompilerParams(vmem_limit_bytes=60000 * 1024),
        name="inverse",
    )(turned, eigvec_y)


def solution(mesh):
    placed = (P("tm", "space", None, None), P(), P(), P(), P(), P(), P())
    return jax.shard_map(
        shards, mesh=mesh, in_specs=placed, out_specs=P("tm", "space", None, None), check_vma=False
    )
```
